256 devices in a mesh: strip: 256 (over x, z, y, core).
Axes of the slice: x: 4, y: 4, z: 8, core: 2. Of those that a mesh axis runs over, the one named last changes fastest.
Arguments:
- features: bfloat16 [64, 8192, 1024], P(None, 'strip'), may hold values from -6 to 6
- row_kernel: bfloat16 [8, 8, 8, 129], replicated, may hold values from -0.1875 to 0.1875
- mix_weight: bfloat16 [64, 64], replicated, may hold values from -0.75 to 0.75
- channel_bias: float32 [64], replicated, may hold values from -3 to 3
Outputs:
- layer_out: bfloat16 [64, 8192, 1024], P(None, 'strip')
The draws below stay inside these ranges and needn't reach their ends.
All inputs are finite; a program needn't handle non-finite values.
Results may differ from the reference program's by a relative error of at most 0.001.
Values may be sent and summed in bfloat16 or wider, within the bound.
A program may use at most 128 MiB of HBM per device.

```python
import jax
import jax.numpy as jnp
from jax import lax

C = 64
GW = 8
HALF = 64
ROWS_DEV = 32
NCOL = 1024
TAPS = 129
GROUPS = 8
ROWS = 8192
N_STRIP = 256


def block_scale(key, extent, split, smallest, largest):
    loudness, own = 1.0, jax.random.fold_in(key, 6)
    for position, shards_of in split:
        heights = jnp.exp(jax.random.uniform(jax.random.fold_in(own, position), (shards_of,), jnp.float32, smallest / len(split), largest / len(split)))
        loudness = loudness * jnp.repeat(heights, extent[position] // shards_of).reshape([-1 if axis == position else 1 for axis in range(len(extent))])
    return loudness


def bell_draw(own_key, dims, deviation, most, cuts=(), dtype=jnp.bfloat16):
    loudness = block_scale(own_key, dims, cuts, -0.22, 0.18) if cuts else 1.0
    drawn = jax.random.normal(own_key, dims, jnp.float32) * deviation * loudness
    return jnp.minimum(jnp.maximum(drawn, -most), most).astype(dtype)


def setup_inputs(seed: int = 0) -> dict:
    arg_keys = jax.random.split(jax.random.key(seed), 5)
    return {
        "features": bell_draw(arg_keys[0], (C, ROWS, NCOL), 1.0, 6.0, ((1, 256),)),
        "row_kernel": bell_draw(arg_keys[1], (GROUPS, GW, GW, TAPS), (GW * TAPS) ** -0.5, 0.1875),
        "mix_weight": bell_draw(arg_keys[2], (C, C), C ** -0.5, 0.75),
        "channel_bias": bell_draw(arg_keys[3], (C,), 0.5, 3.0, (), jnp.float32),
    }


def reference(features, row_kernel, mix_weight, channel_bias):
    grid_rows = ROWS_DEV * N_STRIP
    tap_count = 2 * HALF + 1
    front = row_kernel[..., HALF::-1]
    back = row_kernel[..., 2 * HALF:HALF:-1]
    middle = jnp.zeros((GROUPS, GW, GW, grid_rows - tap_count), jnp.bfloat16)
    filters = jnp.concatenate([front, middle, back], axis=-1).astype(jnp.float32)
    spectra = jnp.fft.rfft(filters, axis=-1)
    grouped = features.astype(jnp.float32).reshape(GROUPS, GW, grid_rows, NCOL)

    def one_group(pair):
        block, spectrum = pair
        block_hat = jnp.fft.rfft(block, axis=1)
        out_hat = jnp.einsum("oif,ifw->ofw", spectrum, block_hat)
        return jnp.fft.irfft(out_hat, n=grid_rows, axis=1)

    conv = lax.map(one_group, (grouped, spectra)).reshape(C, grid_rows, NCOL)
    mixed = jnp.einsum("io,irw->orw", mix_weight.astype(jnp.float32), features.astype(jnp.float32))
    total = conv + mixed + channel_bias[:, None, None]
    return jax.nn.gelu(total).astype(jnp.bfloat16)
```

```python
import functools

import jax
import jax.numpy as jnp
from jax import lax
from jax.experimental import pallas as pl
from jax.experimental.pallas import tpu as pltpu
from jax.sharding import PartitionSpec as P

MESH = pl.DeviceIdType.MESH
LANES = 128
TAIL = 4


def kernel(
    n,
    feat,
    taps_in,
    mix_in,
    bias,
    out,
    x,
    taps_raw,
    taps,
    mix,
    band,
    kron,
    spread,
    mixed,
    local_sem,
    own_sem,
    up_send,
    up_recv,
    down_send,
    down_recv,
    side_send,
    side_recv,
    pass_send,
    pass_recv,
):
    channels, strip, columns = feat.shape
    groups, width, _, tap_count = taps_in.shape
    strips = x.shape[1]
    me = lax.axis_index("strip")
    core = lax.rem(me, 2)
    partner = me + 1 - 2 * core
    ahead, behind = lax.rem(me + 2, n), lax.rem(me + n - 2, n)

    def own_copy(g):
        rows = pl.ds(g * width, width)
        return pltpu.make_async_copy(feat.at[rows], x.at[rows, 2], own_sem.at[g])

    for g in range(groups):
        own_copy(g).start()
    small = [
        pltpu.make_async_copy(taps_in, taps_raw, local_sem.at[0]),
        pltpu.make_async_copy(mix_in, mix, local_sem.at[1]),
    ]
    for copy in small:
        copy.start()

    barrier = pltpu.get_barrier_semaphore()
    for device in (ahead, behind, partner):
        pl.semaphore_signal(barrier, inc=1, device_id=(device,), device_id_type=MESH)
    pl.semaphore_wait(barrier, 3)

    wide = [(g * width, 0, columns, g) for g in range(groups - 1)]
    piece = columns // TAIL
    tail = [((groups - 1) * width, q * piece, piece, groups - 1 + q) for q in range(TAIL)]

    def remote(part, source, target, send, recv, device):
        first, column, size, slot = part
        rows, cols = pl.ds(first, width), pl.ds(column, size)
        return pltpu.make_async_remote_copy(
            src_ref=x.at[rows, source, :, cols],
            dst_ref=x.at[rows, target, :, cols],
            send_sem=send.at[slot],
            recv_sem=recv.at[slot],
            device_id=(device,),
            device_id_type=MESH,
        )

    def up(part):
        return remote(part, 2, 0, up_send, up_recv, ahead)

    def down(part):
        return remote(part, 2, 4, down_send, down_recv, behind)

    def side(part):
        return remote(part, 2, 1 + 2 * core, side_send, side_recv, partner)

    def passed(part):
        return remote(part, 4 - 4 * core, 3 - 2 * core, pass_send, pass_recv, partner)

    for part in wide + tail:
        if part[1] == 0:
            own_copy(part[3]).wait()
        up(part).start()
        down(part).start()
        side(part).start()

    for copy in small:
        copy.wait()
    taps[...] = jnp.zeros_like(taps)
    taps[:, :, :, 0:tap_count] = taps_raw[...].astype(jnp.float32)
    spread_channel = lax.broadcasted_iota(jnp.int32, spread.shape, 0)
    spread_column = lax.broadcasted_iota(jnp.int32, spread.shape, 1)
    spread[...] = jnp.where(spread_column // strip == spread_channel, 1.0, 0.0).astype(spread.dtype)

    span = strips * strip
    rows_out = width * strip
    period = taps.shape[-1]

    def build(g):
        for o in range(width):
            tiles = [None] * (width * span // LANES)
            for i in range(width):
                row = taps[g, o, pl.ds(i, 1), :]
                start = i * span
                rolled = pltpu.roll(
                    jnp.broadcast_to(row, (strip, period)),
                    start % LANES,
                    1,
                    stride=1,
                    stride_axis=0,
                )
                for half in range(period // LANES):
                    at = start // LANES + half
                    block = rolled[:, half * LANES : (half + 1) * LANES]
                    if at < len(tiles):
                        tiles[at] = block if tiles[at] is None else tiles[at] + block
            for at, block in enumerate(tiles):
                band[pl.ds(o * strip, strip), pl.ds(at * LANES, LANES)] = block.astype(band.dtype)
        out_row = lax.broadcasted_iota(jnp.int32, (rows_out, channels), 0)
        out_channel = lax.broadcasted_iota(jnp.int32, (rows_out, channels), 1)
        pick = jnp.where(out_row // strip + g * width == out_channel, 1.0, 0.0).astype(mix.dtype)
        picked = lax.dot_general(
            pick, mix[...], (((1,), (1,)), ((), ())), preferred_element_type=jnp.float32
        ).astype(mix.dtype)
        step = 2 * LANES
        for c in range(0, channels * strip, step):
            full = jnp.dot(picked, spread[:, c : c + step], preferred_element_type=jnp.float32)
            p = lax.broadcasted_iota(jnp.int32, full.shape, 0) % strip
            t = lax.broadcasted_iota(jnp.int32, full.shape, 1) % strip
            kron[:, c : c + step] = jnp.where(p == t, full, 0.0).astype(kron.dtype)

        @pl.loop(0, columns // piece)
        def _(q):
            cols = pl.ds(pl.multiple_of(q * piece, piece), piece)
            data = x[:, 2, :, cols].reshape(channels * strip, piece)
            mixed[:, cols] = jnp.dot(kron[...], data, preferred_element_type=jnp.float32)

    def finish(g, cols):
        data = x[pl.ds(g * width, width), :, :, cols].reshape(width * span, piece)
        conv = jnp.dot(band[...], data, preferred_element_type=jnp.float32)
        total = conv + mixed[:, cols]
        for o in range(width):
            c = g * width + o
            value = jax.nn.gelu(total[o * strip : (o + 1) * strip] + bias[c])
            out[c, :, cols] = value.astype(out.dtype)

    @pl.loop(0, groups - 1)
    def _(g):
        build(g)
        part = (g * width, 0, columns, g)
        up(part).wait_recv()
        down(part).wait_recv()
        passed(part).start()
        side(part).wait_recv()
        passed(part).wait_recv()

        @pl.loop(0, columns // piece)
        def _(q):
            finish(g, pl.ds(pl.multiple_of(q * piece, piece), piece))

    last = groups - 1
    build(last)
    for q, part in enumerate(tail):
        up(part).wait_recv()
        down(part).wait_recv()
        passed(part).start()
        if q > 0:
            side(tail[q - 1]).wait_recv()
            passed(tail[q - 1]).wait_recv()
            finish(last, pl.ds((q - 1) * piece, piece))
    side(tail[-1]).wait_recv()
    passed(tail[-1]).wait_recv()
    finish(last, pl.ds((TAIL - 1) * piece, piece))

    for part in wide + tail:
        up(part).wait_send()
        down(part).wait_send()
        side(part).wait_send()
        passed(part).wait_send()


def local(n, features, row_kernel, mix_weight, channel_bias):
    channels, strip, columns = features.shape
    groups, width, _, tap_count = row_kernel.shape
    strips = (tap_count - 1) // strip + 1
    period = -(-(strips * strip + 3 * strip) // LANES) * LANES
    slots = groups - 1 + TAIL
    hbm = pl.BlockSpec(memory_space=pl.ANY)
    return pl.pallas_call(
        functools.partial(kernel, n),
        out_shape=jax.ShapeDtypeStruct(features.shape, jnp.bfloat16),
        in_specs=[hbm, hbm, hbm, pl.BlockSpec(memory_space=pltpu.SMEM)],
        out_specs=pl.BlockSpec(memory_space=pltpu.VMEM),
        scratch_shapes=[
            pltpu.VMEM((channels, strips, strip, columns), jnp.bfloat16),
            pltpu.VMEM(row_kernel.shape, jnp.bfloat16),
            pltpu.VMEM((groups, width, width, period), jnp.float32),
            pltpu.VMEM(mix_weight.shape, jnp.bfloat16),
            pltpu.VMEM((width * strip, width * strips * strip), jnp.bfloat16),
            pltpu.VMEM((width * strip, channels * strip), jnp.bfloat16),
            pltpu.VMEM((channels, channels * strip), jnp.bfloat16),
            pltpu.VMEM((width * strip, columns), jnp.float32),
            pltpu.SemaphoreType.DMA((2,)),
            pltpu.SemaphoreType.DMA((groups,)),
        ]
        + [pltpu.SemaphoreType.DMA((slots,))] * 8,
        compiler_params=pltpu.CompilerParams(
            collective_id=0, has_side_effects=True, vmem_limit_bytes=48 * 2**20
        ),
    )(features, row_kernel, mix_weight, channel_bias)


def solution(mesh):
    return jax.shard_map(
        functools.partial(local, mesh.shape["strip"]),
        mesh=mesh,
        in_specs=(P(None, "strip", None), P(), P(), P()),
        out_specs=P(None, "strip", None),
        check_vma=False,
    )
```

```python
import functools

import jax
import jax.numpy as jnp
from jax import lax
from jax.experimental import pallas as pl
from jax.experimental.pallas import tpu as pltpu
from jax.sharding import PartitionSpec as P

MESH = pl.DeviceIdType.MESH
LANES = 128
TAIL = 384, 384, 256
TILE = 512
LEAD = 3
SLAB = 32
LINE = 4


def kernel(
    n,
    feat,
    taps_in,
    mix_in,
    bias_in,
    out,
    x,
    taps_raw,
    taps,
    mix,
    bias,
    band,
    kron,
    spread,
    mixed,
    landing,
    local_sem,
    own_sem,
    flow_send,
    flow_recv,
    side_send,
    side_recv,
    pass_send,
    pass_recv,
    land_send,
    land_recv,
    ready,
):
    channels, strip, columns = feat.shape
    groups, width, _, tap_count = taps_in.shape
    strips = x.shape[1]
    me = lax.axis_index("strip")
    core = lax.rem(me, 2)
    partner = me + 1 - 2 * core
    ahead, behind = lax.rem(me + 2, n), lax.rem(me + n - 2, n)
    place = lax.rem(lax.div(me, 2), SLAB)
    first = (place == 0).astype(jnp.int32)
    last_chip = (place == SLAB - 1).astype(jnp.int32)
    step = 2 * (SLAB - LINE)
    relays_up = (place * 2 == step).astype(jnp.int32)
    relays_down = ((SLAB - 1 - place) * 2 == step).astype(jnp.int32)

    def wrapped(device):
        return lax.rem(device + n, n)

    def own_copy(g):
        rows = pl.ds(g * width, width)
        return pltpu.make_async_copy(feat.at[rows], x.at[rows, 2], own_sem.at[g])

    for g in [groups - 1] + list(range(groups - 1)):
        own_copy(g).start()
    small = [
        pltpu.make_async_copy(taps_in, taps_raw, local_sem.at[0]),
        pltpu.make_async_copy(mix_in, mix, local_sem.at[1]),
        pltpu.make_async_copy(bias_in, bias, local_sem.at[2]),
    ]
    for copy in small:
        copy.start()

    barrier = pltpu.get_barrier_semaphore()

    def greet(device):
        pl.semaphore_signal(barrier, inc=1, device_id=(device,), device_id_type=MESH)

    greet(behind)
    greet(partner)

    @pl.when(last_chip == 0)
    def _():
        greet(ahead)

    @pl.when(first == 1)
    def _():
        greet(me + step)

    @pl.when(relays_up == 1)
    def _():
        greet(wrapped(me - step - 2))

    @pl.when(relays_down == 1)
    def _():
        greet(me + step)
        greet(wrapped(me + step + 2))

    pl.semaphore_wait(barrier, 3 + 2 * last_chip + relays_up)

    @pl.when(last_chip == 1)
    def _():
        for device in (ahead, me - step):
            pl.semaphore_signal(ready, inc=1, device_id=(device,), device_id_type=MESH)

    wide = [(g * width, 0, columns, g) for g in range(groups - 1)]
    last = groups - 1
    tail = [(last * width, sum(TAIL[:q]), size, last + q) for q, size in enumerate(TAIL)]
    relayed = tail[0]

    def block(part, strip_at):
        first_channel, column, size, _ = part
        return x.at[pl.ds(first_channel, width), strip_at, :, pl.ds(column, size)]

    def remote(source, target, send, recv, device):
        return pltpu.make_async_remote_copy(
            src_ref=source,
            dst_ref=target,
            send_sem=send,
            recv_sem=recv,
            device_id=(device,),
            device_id_type=MESH,
        )

    def flow(part, way):
        device = ahead + way * (behind - ahead)
        sems = flow_send.at[way, part[3]], flow_recv.at[way, part[3]]
        return remote(block(part, 2), block(part, 4 * way), *sems, device)

    def side(part):
        sems = side_send.at[part[3]], side_recv.at[part[3]]
        return remote(block(part, 2), block(part, 1 + 2 * core), *sems, partner)

    def passed(part):
        sems = pass_send.at[part[3]], pass_recv.at[part[3]]
        return remote(block(part, 4 - 4 * core), block(part, 3 - 2 * core), *sems, partner)

    def to_relay(way):
        device = wrapped(ahead + step) if way == 0 else wrapped(behind - step)
        return remote(block(relayed, 2), landing, flow_send.at[way, relayed[3]], land_recv, device)

    def from_relay(way):
        target = block(relayed, 4 * way)
        return remote(landing, target, land_send, flow_recv.at[way, relayed[3]], me + (2 * way - 1) * step)

    def start_tail(way):
        @pl.when(last_chip * (1 - way) + first * way == 0)
        def _():
            flow(relayed, way).start()

        for part in tail[1:]:
            flow(part, way).start()

    own_copy(last).wait()
    for to, sender in enumerate((last_chip, first)):

        @pl.when(sender == 1)
        def _():
            to_relay(to).start()

    way = (1 - core) * (1 - first)
    for part in wide[:LEAD]:
        own_copy(part[3]).wait()
        flow(part, way).start()
    for part in wide[:LEAD]:
        side(part).start()
    for part in wide[LEAD:]:
        own_copy(part[3]).wait()

    for copy in small:
        copy.wait()
    taps[...] = jnp.zeros_like(taps)
    taps[:, :, :, 0:tap_count] = taps_raw[...].astype(jnp.float32)
    spread_channel = lax.broadcasted_iota(jnp.int32, spread.shape, 0)
    spread_column = lax.broadcasted_iota(jnp.int32, spread.shape, 1)
    spread[...] = jnp.where(spread_column // strip == spread_channel, 1.0, 0.0).astype(spread.dtype)

    @pl.when(first == 1)
    def _():
        pl.semaphore_wait(ready, 1)

    for part in wide[:LEAD]:
        flow(part, 1 - way).start()

    for to, relays in enumerate((relays_up, relays_down)):

        @pl.when(relays == 1)
        def _():
            if to == 1:
                pl.semaphore_wait(ready, 1)
            to_relay(to).wait_recv()
            from_relay(to).start()

    span = strips * strip
    rows_out = width * strip
    period = taps.shape[-1]

    def build(g):
        for o in range(width):
            tiles = [None] * (width * span // LANES)
            for i in range(width):
                row = taps[g, o, pl.ds(i, 1), :]
                start = i * span
                rolled = pltpu.roll(
                    jnp.broadcast_to(row, (strip, period)),
                    start % LANES,
                    1,
                    stride=1,
                    stride_axis=0,
                )
                for half in range(period // LANES):
                    at = start // LANES + half
                    tile = rolled[:, half * LANES : (half + 1) * LANES]
                    if at < len(tiles):
                        tiles[at] = tile if tiles[at] is None else tiles[at] + tile
            for at, tile in enumerate(tiles):
                band[pl.ds(o * strip, strip), pl.ds(at * LANES, LANES)] = tile.astype(band.dtype)
        out_row = lax.broadcasted_iota(jnp.int32, (rows_out, channels), 0)
        out_channel = lax.broadcasted_iota(jnp.int32, (rows_out, channels), 1)
        pick = jnp.where(out_row // strip + g * width == out_channel, 1.0, 0.0).astype(mix.dtype)
        picked = lax.dot_general(
            pick, mix[...], (((1,), (1,)), ((), ())), preferred_element_type=jnp.float32
        ).astype(mix.dtype)
        step = 2 * LANES
        for c in range(0, channels * strip, step):
            full = jnp.dot(picked, spread[:, c : c + step], preferred_element_type=jnp.float32)
            p = lax.broadcasted_iota(jnp.int32, full.shape, 0) % strip
            t = lax.broadcasted_iota(jnp.int32, full.shape, 1) % strip
            kron[:, c : c + step] = jnp.where(p == t, full, 0.0).astype(kron.dtype)

        @pl.loop(0, columns // TILE)
        def _(q):
            cols = pl.ds(pl.multiple_of(q * TILE, TILE), TILE)
            data = x[:, 2, :, cols].reshape(channels * strip, TILE)
            mixed[:, cols] = jnp.dot(kron[...], data, preferred_element_type=jnp.float32)

    def finish(g, column, size):
        cols = pl.ds(column, size)
        data = x[pl.ds(g * width, width), :, :, cols].reshape(width * span, size)
        conv = jnp.dot(band[...], data, preferred_element_type=jnp.float32)
        total = conv + mixed[:, cols]
        for o in range(width):
            c = g * width + o
            value = jax.nn.gelu(total[o * strip : (o + 1) * strip] + bias[c])
            out[c, :, cols] = value.astype(out.dtype)

    @pl.loop(0, groups - 1)
    def _(g):
        build(g)
        part = (g * width, 0, columns, g)
        flow(part, 0).wait_recv()
        flow(part, 1).wait_recv()
        passed(part).start()

        @pl.when(g + LEAD < groups - 1)
        def _():
            later = ((g + LEAD) * width, 0, columns, g + LEAD)
            flow(later, way).start()
            flow(later, 1 - way).start()
            side(later).start()

        @pl.when(g + LEAD == groups - 1)
        def _():
            start_tail(way)
            start_tail(1 - way)
            for later in tail:
                side(later).start()

        side(part).wait_recv()
        passed(part).wait_recv()

        @pl.loop(0, columns // TILE)
        def _(q):
            finish(g, pl.multiple_of(q * TILE, TILE), TILE)

    build(last)
    for q, part in enumerate(tail):
        flow(part, 0).wait_recv()
        flow(part, 1).wait_recv()
        passed(part).start()
        if q > 0:
            side(tail[q - 1]).wait_recv()
            passed(tail[q - 1]).wait_recv()
            finish(last, *tail[q - 1][1:3])
    side(tail[-1]).wait_recv()
    passed(tail[-1]).wait_recv()
    finish(last, *tail[-1][1:3])

    for part in wide + tail:
        flow(part, 0).wait_send()
        flow(part, 1).wait_send()
        side(part).wait_send()
        passed(part).wait_send()

    @pl.when(relays_up + relays_down == 1)
    def _():
        from_relay(0).wait_send()


def local(n, features, row_kernel, mix_weight, channel_bias):
    channels, strip, columns = features.shape
    groups, width, _, tap_count = row_kernel.shape
    strips = (tap_count - 1) // strip + 1
    period = -(-(strips * strip + 3 * strip) // LANES) * LANES
    slots = groups - 1 + len(TAIL)
    small = row_kernel, mix_weight, channel_bias
    hbm = pl.BlockSpec(memory_space=pltpu.HBM)
    return pl.pallas_call(
        functools.partial(kernel, n),
        out_shape=jax.ShapeDtypeStruct(features.shape, jnp.bfloat16),
        in_specs=[hbm, hbm, hbm, hbm],
        out_specs=pl.BlockSpec(memory_space=pltpu.VMEM),
        scratch_shapes=[
            pltpu.VMEM((channels, strips, strip, columns), jnp.bfloat16),
            pltpu.VMEM(row_kernel.shape, jnp.bfloat16),
            pltpu.VMEM((groups, width, width, period), jnp.float32),
            pltpu.VMEM(mix_weight.shape, jnp.bfloat16),
            pltpu.SMEM(channel_bias.shape, jnp.float32),
            pltpu.VMEM((width * strip, width * strips * strip), jnp.bfloat16),
            pltpu.VMEM((width * strip, channels * strip), jnp.bfloat16),
            pltpu.VMEM((channels, channels * strip), jnp.bfloat16),
            pltpu.VMEM((width * strip, columns), jnp.float32),
            pltpu.VMEM((width, strip, TAIL[0]), jnp.bfloat16),
            pltpu.SemaphoreType.DMA((3,)),
            pltpu.SemaphoreType.DMA((groups,)),
        ]
        + [pltpu.SemaphoreType.DMA((2, slots))] * 2
        + [pltpu.SemaphoreType.DMA((slots,))] * 4
        + [pltpu.SemaphoreType.DMA] * 2
        + [pltpu.SemaphoreType.REGULAR],
        compiler_params=pltpu.CompilerParams(
            collective_id=0, has_side_effects=True, vmem_limit_bytes=48 * 2**20
        ),
    )(features, *(pltpu.with_memory_space_constraint(a, pltpu.HBM) for a in small))


def solution(mesh):
    return jax.shard_map(
        functools.partial(local, mesh.shape["strip"]),
        mesh=mesh,
        in_specs=(P(None, "strip", None), P(), P(), P()),
        out_specs=P(None, "strip", None),
        check_vma=False,
    )
```

```python
import functools

import jax
import jax.numpy as jnp
from jax import lax
from jax.experimental import pallas as pl
from jax.experimental.pallas import tpu as pltpu
from jax.sharding import PartitionSpec as P

MESH = pl.DeviceIdType.MESH
LANES = 128
TAIL = 256, 256, 512
RELAYS = 2
TILE = 512
LEAD = 3
SLAB = 32
LINE = 4


def kernel(
    n,
    feat,
    taps_in,
    mix_in,
    bias_in,
    out,
    x,
    taps_raw,
    taps,
    mix,
    bias,
    band,
    kron,
    spread,
    mixed,
    landing,
    local_sem,
    own_sem,
    flow_send,
    flow_recv,
    side_send,
    side_recv,
    pass_send,
    pass_recv,
    land_send,
    land_recv,
    ready,
    settled,
):
    channels, strip, columns = feat.shape
    groups, width, _, tap_count = taps_in.shape
    strips = x.shape[1]
    me = lax.axis_index("strip")
    core = lax.rem(me, 2)
    partner = me + 1 - 2 * core
    ahead, behind = lax.rem(me + 2, n), lax.rem(me + n - 2, n)
    place = lax.rem(lax.div(me, 2), SLAB)
    first = (place == 0).astype(jnp.int32)
    last_chip = (place == SLAB - 1).astype(jnp.int32)
    steps = [2 * (SLAB - LINE * (j + 1)) for j in range(RELAYS)]
    relays_up = [(place * 2 == step).astype(jnp.int32) for step in steps]
    relays_down = [((SLAB - 1 - place) * 2 == step).astype(jnp.int32) for step in steps]

    def wrapped(device):
        return lax.rem(device + n, n)

    def own_copy(g):
        rows = pl.ds(g * width, width)
        return pltpu.make_async_copy(feat.at[rows], x.at[rows, 2], own_sem.at[g])

    for g in [groups - 1] + list(range(groups - 1)):
        own_copy(g).start()
    small = [
        pltpu.make_async_copy(taps_in, taps_raw, local_sem.at[0]),
        pltpu.make_async_copy(mix_in, mix, local_sem.at[1]),
        pltpu.make_async_copy(bias_in, bias, local_sem.at[2]),
    ]
    for copy in small:
        copy.start()

    barrier = pltpu.get_barrier_semaphore()

    def greet(device):
        pl.semaphore_signal(barrier, inc=1, device_id=(device,), device_id_type=MESH)

    greet(behind)
    greet(partner)

    @pl.when(last_chip == 0)
    def _():
        greet(ahead)

    for j, step in enumerate(steps):

        @pl.when(first == 1)
        def _():
            greet(me + step)
            if j > 0:
                greet(wrapped(me - step - 2))

        @pl.when(relays_up[j] == 1)
        def _():
            greet(wrapped(me - step - 2))

        @pl.when(relays_down[j] == 1)
        def _():
            greet(me + step)
            if j == 0:
                greet(wrapped(me + step + 2))

    pl.semaphore_wait(barrier, 3 + 2 * RELAYS * last_chip + sum(relays_up) + sum(relays_down[1:]))

    @pl.when(last_chip == 1)
    def _():
        for device in [ahead] + [me - step for step in steps]:
            pl.semaphore_signal(ready, inc=1, device_id=(device,), device_id_type=MESH)

    for j, step in list(enumerate(steps))[1:]:

        @pl.when(relays_down[j] == 1)
        def _():
            device = wrapped(me + step + 2)
            pl.semaphore_signal(settled, inc=1, device_id=(device,), device_id_type=MESH)

    wide = [(g * width, 0, columns, g) for g in range(groups - 1)]
    last = groups - 1
    tail = [(last * width, sum(TAIL[:q]), size, last + q) for q, size in enumerate(TAIL)]
    relayed = tail[:RELAYS]

    def block(part, strip_at):
        first_channel, column, size, _ = part
        return x.at[pl.ds(first_channel, width), strip_at, :, pl.ds(column, size)]

    def remote(source, target, send, recv, device):
        return pltpu.make_async_remote_copy(
            src_ref=source,
            dst_ref=target,
            send_sem=send,
            recv_sem=recv,
            device_id=(device,),
            device_id_type=MESH,
        )

    def flow(part, way):
        device = ahead + way * (behind - ahead)
        sems = flow_send.at[way, part[3]], flow_recv.at[way, part[3]]
        return remote(block(part, 2), block(part, 4 * way), *sems, device)

    def side(part):
        sems = side_send.at[part[3]], side_recv.at[part[3]]
        return remote(block(part, 2), block(part, 1 + 2 * core), *sems, partner)

    def passed(part):
        sems = pass_send.at[part[3]], pass_recv.at[part[3]]
        return remote(block(part, 4 - 4 * core), block(part, 3 - 2 * core), *sems, partner)

    def to_relay(way, j):
        part = relayed[j]
        device = wrapped(ahead + steps[j]) if way == 0 else wrapped(behind - steps[j])
        return remote(block(part, 2), landing, flow_send.at[way, part[3]], land_recv, device)

    def from_relay(way, j):
        part = relayed[j]
        device = me + (2 * way - 1) * steps[j]
        return remote(landing, block(part, 4 * way), land_send, flow_recv.at[way, part[3]], device)

    def start_tail(way):
        @pl.when(last_chip * (1 - way) + first * way == 0)
        def _():
            for part in relayed:
                flow(part, way).start()

        for part in tail[RELAYS:]:
            flow(part, way).start()

    own_copy(last).wait()

    @pl.when(last_chip == 1)
    def _():
        for j in range(RELAYS):
            to_relay(0, j).start()

    @pl.when(first == 1)
    def _():
        to_relay(1, 0).start()

    way = (1 - core) * (1 - first)
    for part in wide[:LEAD]:
        own_copy(part[3]).wait()
        flow(part, way).start()
    for part in wide[:LEAD]:
        side(part).start()
    for part in wide[LEAD:]:
        own_copy(part[3]).wait()

    @pl.when(first == 1)
    def _():
        pl.semaphore_wait(settled, RELAYS - 1)
        for j in range(1, RELAYS):
            to_relay(1, j).start()

    for copy in small:
        copy.wait()
    taps[...] = jnp.zeros_like(taps)
    taps[:, :, :, 0:tap_count] = taps_raw[...].astype(jnp.float32)
    spread_channel = lax.broadcasted_iota(jnp.int32, spread.shape, 0)
    spread_column = lax.broadcasted_iota(jnp.int32, spread.shape, 1)
    spread[...] = jnp.where(spread_column // strip == spread_channel, 1.0, 0.0).astype(spread.dtype)

    @pl.when(first == 1)
    def _():
        pl.semaphore_wait(ready, 1)

    for part in wide[:LEAD]:
        flow(part, 1 - way).start()

    for to, relays in enumerate((relays_up, relays_down)):
        for j in range(RELAYS):

            @pl.when(relays[j] == 1)
            def _():
                if to == 1:
                    pl.semaphore_wait(ready, 1)
                to_relay(to, j).wait_recv()
                from_relay(to, j).start()

    span = strips * strip
    rows_out = width * strip
    period = taps.shape[-1]

    def build(g):
        for o in range(width):
            tiles = [None] * (width * span // LANES)
            for i in range(width):
                row = taps[g, o, pl.ds(i, 1), :]
                start = i * span
                rolled = pltpu.roll(
                    jnp.broadcast_to(row, (strip, period)),
                    start % LANES,
                    1,
                    stride=1,
                    stride_axis=0,
                )
                for half in range(period // LANES):
                    at = start // LANES + half
                    tile = rolled[:, half * LANES : (half + 1) * LANES]
                    if at < len(tiles):
                        tiles[at] = tile if tiles[at] is None else tiles[at] + tile
            for at, tile in enumerate(tiles):
                band[pl.ds(o * strip, strip), pl.ds(at * LANES, LANES)] = tile.astype(band.dtype)
        out_row = lax.broadcasted_iota(jnp.int32, (rows_out, channels), 0)
        out_channel = lax.broadcasted_iota(jnp.int32, (rows_out, channels), 1)
        pick = jnp.where(out_row // strip + g * width == out_channel, 1.0, 0.0).astype(mix.dtype)
        picked = lax.dot_general(
            pick, mix[...], (((1,), (1,)), ((), ())), preferred_element_type=jnp.float32
        ).astype(mix.dtype)
        step = 2 * LANES
        for c in range(0, channels * strip, step):
            full = jnp.dot(picked, spread[:, c : c + step], preferred_element_type=jnp.float32)
            p = lax.broadcasted_iota(jnp.int32, full.shape, 0) % strip
            t = lax.broadcasted_iota(jnp.int32, full.shape, 1) % strip
            kron[:, c : c + step] = jnp.where(p == t, full, 0.0).astype(kron.dtype)

        @pl.loop(0, columns // TILE)
        def _(q):
            cols = pl.ds(pl.multiple_of(q * TILE, TILE), TILE)
            data = x[:, 2, :, cols].reshape(channels * strip, TILE)
            mixed[:, cols] = jnp.dot(kron[...], data, preferred_element_type=jnp.float32)

    def finish(g, column, size):
        cols = pl.ds(column, size)
        data = x[pl.ds(g * width, width), :, :, cols].reshape(width * span, size)
        conv = jnp.dot(band[...], data, preferred_element_type=jnp.float32)
        total = conv + mixed[:, cols]
        for o in range(width):
            c = g * width + o
            value = jax.nn.gelu(total[o * strip : (o + 1) * strip] + bias[c])
            out[c, :, cols] = value.astype(out.dtype)

    @pl.loop(0, groups - 1)
    def _(g):
        build(g)
        part = (g * width, 0, columns, g)
        flow(part, 0).wait_recv()
        flow(part, 1).wait_recv()
        passed(part).start()

        @pl.when(g + LEAD < groups - 1)
        def _():
            later = ((g + LEAD) * width, 0, columns, g + LEAD)
            flow(later, way).start()
            flow(later, 1 - way).start()
            side(later).start()

        @pl.when(g + LEAD == groups - 1)
        def _():
            start_tail(way)
            start_tail(1 - way)
            for later in tail:
                side(later).start()

        side(part).wait_recv()
        passed(part).wait_recv()

        @pl.loop(0, columns // TILE)
        def _(q):
            finish(g, pl.multiple_of(q * TILE, TILE), TILE)

    build(last)
    for q, part in enumerate(tail):
        flow(part, 0).wait_recv()
        flow(part, 1).wait_recv()
        passed(part).start()
        if q > 0:
            side(tail[q - 1]).wait_recv()
            passed(tail[q - 1]).wait_recv()
            finish(last, *tail[q - 1][1:3])
    side(tail[-1]).wait_recv()
    passed(tail[-1]).wait_recv()
    finish(last, *tail[-1][1:3])

    for part in wide + tail:
        flow(part, 0).wait_send()
        flow(part, 1).wait_send()
        side(part).wait_send()
        passed(part).wait_send()

    @pl.when(sum(relays_up) + sum(relays_down) == 1)
    def _():
        from_relay(0, 0).wait_send()


def local(n, features, row_kernel, mix_weight, channel_bias):
    channels, strip, columns = features.shape
    groups, width, _, tap_count = row_kernel.shape
    strips = (tap_count - 1) // strip + 1
    period = -(-(strips * strip + 3 * strip) // LANES) * LANES
    slots = groups - 1 + len(TAIL)
    small = row_kernel, mix_weight, channel_bias
    hbm = pl.BlockSpec(memory_space=pltpu.HBM)
    return pl.pallas_call(
        functools.partial(kernel, n),
        out_shape=jax.ShapeDtypeStruct(features.shape, jnp.bfloat16),
        in_specs=[hbm, hbm, hbm, hbm],
        out_specs=pl.BlockSpec(memory_space=pltpu.VMEM),
        scratch_shapes=[
            pltpu.VMEM((channels, strips, strip, columns), jnp.bfloat16),
            pltpu.VMEM(row_kernel.shape, jnp.bfloat16),
            pltpu.VMEM((groups, width, width, period), jnp.float32),
            pltpu.VMEM(mix_weight.shape, jnp.bfloat16),
            pltpu.SMEM(channel_bias.shape, jnp.float32),
            pltpu.VMEM((width * strip, width * strips * strip), jnp.bfloat16),
            pltpu.VMEM((width * strip, channels * strip), jnp.bfloat16),
            pltpu.VMEM((channels, channels * strip), jnp.bfloat16),
            pltpu.VMEM((width * strip, columns), jnp.float32),
            pltpu.VMEM((width, strip, TAIL[0]), jnp.bfloat16),
            pltpu.SemaphoreType.DMA((3,)),
            pltpu.SemaphoreType.DMA((groups,)),
        ]
        + [pltpu.SemaphoreType.DMA((2, slots))] * 2
        + [pltpu.SemaphoreType.DMA((slots,))] * 4
        + [pltpu.SemaphoreType.DMA] * 2
        + [pltpu.SemaphoreType.REGULAR] * 2,
        compiler_params=pltpu.CompilerParams(
            collective_id=0, has_side_effects=True, vmem_limit_bytes=48 * 2**20
        ),
    )(features, *(pltpu.with_memory_space_constraint(a, pltpu.HBM) for a in small))


def solution(mesh):
    return jax.shard_map(
        functools.partial(local, mesh.shape["strip"]),
        mesh=mesh,
        in_specs=(P(None, "strip", None), P(), P(), P()),
        out_specs=P(None, "strip", None),
        check_vma=False,
    )
```

```python
import functools

import jax
import jax.numpy as jnp
from jax import lax
from jax.experimental import pallas as pl
from jax.experimental.pallas import tpu as pltpu
from jax.sharding import PartitionSpec as P

MESH = pl.DeviceIdType.MESH
LANES = 128
TAIL = 384, 256, 384
RELAYS = 2
TILE = 512
LEAD = 3
SLAB = 32
LINE = 4


def kernel(
    n,
    feat,
    taps_in,
    mix_in,
    bias_in,
    out,
    x,
    taps_raw,
    taps,
    mix,
    bias,
    band,
    kron,
    spread,
    mixed,
    landing,
    local_sem,
    own_sem,
    flow_send,
    flow_recv,
    side_send,
    side_recv,
    pass_send,
    pass_recv,
    land_send,
    land_recv,
    ready,
    settled,
):
    channels, strip, columns = feat.shape
    groups, width, _, tap_count = taps_in.shape
    strips = x.shape[1]
    me = lax.axis_index("strip")
    core = lax.rem(me, 2)
    partner = me + 1 - 2 * core
    ahead, behind = lax.rem(me + 2, n), lax.rem(me + n - 2, n)
    place = lax.rem(lax.div(me, 2), SLAB)
    first = (place == 0).astype(jnp.int32)
    last_chip = (place == SLAB - 1).astype(jnp.int32)
    steps = [2 * (SLAB - LINE * (j + 1)) for j in range(RELAYS)]
    relays_up = [(place * 2 == step).astype(jnp.int32) for step in steps]
    relays_down = [((SLAB - 1 - place) * 2 == step).astype(jnp.int32) for step in steps]

    def wrapped(device):
        return lax.rem(device + n, n)

    def own_copy(g):
        rows = pl.ds(g * width, width)
        return pltpu.make_async_copy(feat.at[rows], x.at[rows, 2], own_sem.at[g])

    for g in [groups - 1] + list(range(groups - 1)):
        own_copy(g).start()
    small = [
        pltpu.make_async_copy(taps_in, taps_raw, local_sem.at[0]),
        pltpu.make_async_copy(mix_in, mix, local_sem.at[1]),
        pltpu.make_async_copy(bias_in, bias, local_sem.at[2]),
    ]
    for copy in small:
        copy.start()

    barrier = pltpu.get_barrier_semaphore()

    def greet(device):
        pl.semaphore_signal(barrier, inc=1, device_id=(device,), device_id_type=MESH)

    greet(behind)
    greet(partner)

    @pl.when(last_chip == 0)
    def _():
        greet(ahead)

    for j, step in enumerate(steps):

        @pl.when(first == 1)
        def _():
            greet(me + step)
            if j > 0:
                greet(wrapped(me - step - 2))

        @pl.when(relays_up[j] == 1)
        def _():
            greet(wrapped(me - step - 2))

        @pl.when(relays_down[j] == 1)
        def _():
            greet(me + step)
            if j == 0:
                greet(wrapped(me + step + 2))

    pl.semaphore_wait(barrier, 3 + 2 * RELAYS * last_chip + sum(relays_up) + sum(relays_down[1:]))

    @pl.when(last_chip == 1)
    def _():
        for device in [ahead] + [me - step for step in steps]:
            pl.semaphore_signal(ready, inc=1, device_id=(device,), device_id_type=MESH)

    for j, step in list(enumerate(steps))[1:]:

        @pl.when(relays_down[j] == 1)
        def _():
            device = wrapped(me + step + 2)
            pl.semaphore_signal(settled, inc=1, device_id=(device,), device_id_type=MESH)

    wide = [(g * width, 0, columns, g) for g in range(groups - 1)]
    last = groups - 1
    tail = [(last * width, sum(TAIL[:q]), size, last + q) for q, size in enumerate(TAIL)]
    relayed = tail[:RELAYS]

    def block(part, strip_at):
        first_channel, column, size, _ = part
        return x.at[pl.ds(first_channel, width), strip_at, :, pl.ds(column, size)]

    def remote(source, target, send, recv, device):
        return pltpu.make_async_remote_copy(
            src_ref=source,
            dst_ref=target,
            send_sem=send,
            recv_sem=recv,
            device_id=(device,),
            device_id_type=MESH,
        )

    def flow(part, way):
        device = ahead + way * (behind - ahead)
        sems = flow_send.at[way, part[3]], flow_recv.at[way, part[3]]
        return remote(block(part, 2), block(part, 4 * way), *sems, device)

    def side(part):
        sems = side_send.at[part[3]], side_recv.at[part[3]]
        return remote(block(part, 2), block(part, 1 + 2 * core), *sems, partner)

    def passed(part):
        sems = pass_send.at[part[3]], pass_recv.at[part[3]]
        return remote(block(part, 4 - 4 * core), block(part, 3 - 2 * core), *sems, partner)

    def landed(part):
        return landing.at[:, :, pl.ds(0, part[2])]

    def to_relay(way, j):
        part = relayed[j]
        device = wrapped(ahead + steps[j]) if way == 0 else wrapped(behind - steps[j])
        return remote(block(part, 2), landed(part), flow_send.at[way, part[3]], land_recv, device)

    def from_relay(way, j):
        part = relayed[j]
        device = me + (2 * way - 1) * steps[j]
        return remote(landed(part), block(part, 4 * way), land_send, flow_recv.at[way, part[3]], device)

    def start_tail(way):
        @pl.when(last_chip * (1 - way) + first * way == 0)
        def _():
            for part in relayed:
                flow(part, way).start()

        for part in tail[RELAYS:]:
            flow(part, way).start()

    own_copy(last).wait()

    @pl.when(last_chip == 1)
    def _():
        for j in range(RELAYS):
            to_relay(0, j).start()

    @pl.when(first == 1)
    def _():
        to_relay(1, 0).start()

    way = (1 - core) * (1 - first)
    for part in wide[:LEAD]:
        own_copy(part[3]).wait()
        flow(part, way).start()
    for part in wide[:LEAD]:
        side(part).start()
    for part in wide[LEAD:]:
        own_copy(part[3]).wait()

    @pl.when(first == 1)
    def _():
        pl.semaphore_wait(settled, RELAYS - 1)
        for j in range(1, RELAYS):
            to_relay(1, j).start()

    for copy in small:
        copy.wait()
    taps[...] = jnp.zeros_like(taps)
    taps[:, :, :, 0:tap_count] = taps_raw[...].astype(jnp.float32)
    spread_channel = lax.broadcasted_iota(jnp.int32, spread.shape, 0)
    spread_column = lax.broadcasted_iota(jnp.int32, spread.shape, 1)
    spread[...] = jnp.where(spread_column // strip == spread_channel, 1.0, 0.0).astype(spread.dtype)

    @pl.when(first == 1)
    def _():
        pl.semaphore_wait(ready, 1)

    for part in wide[:LEAD]:
        flow(part, 1 - way).start()

    for to, relays in enumerate((relays_up, relays_down)):
        for j in range(RELAYS):

            @pl.when(relays[j] == 1)
            def _():
                if to == 1:
                    pl.semaphore_wait(ready, 1)
                to_relay(to, j).wait_recv()
                from_relay(to, j).start()

    span = strips * strip
    rows_out = width * strip
    period = taps.shape[-1]

    def build(g):
        for o in range(width):
            tiles = [None] * (width * span // LANES)
            for i in range(width):
                row = taps[g, o, pl.ds(i, 1), :]
                start = i * span
                rolled = pltpu.roll(
                    jnp.broadcast_to(row, (strip, period)),
                    start % LANES,
                    1,
                    stride=1,
                    stride_axis=0,
                )
                for half in range(period // LANES):
                    at = start // LANES + half
                    tile = rolled[:, half * LANES : (half + 1) * LANES]
                    if at < len(tiles):
                        tiles[at] = tile if tiles[at] is None else tiles[at] + tile
            for at, tile in enumerate(tiles):
                band[pl.ds(o * strip, strip), pl.ds(at * LANES, LANES)] = tile.astype(band.dtype)
        out_row = lax.broadcasted_iota(jnp.int32, (rows_out, channels), 0)
        out_channel = lax.broadcasted_iota(jnp.int32, (rows_out, channels), 1)
        pick = jnp.where(out_row // strip + g * width == out_channel, 1.0, 0.0).astype(mix.dtype)
        picked = lax.dot_general(
            pick, mix[...], (((1,), (1,)), ((), ())), preferred_element_type=jnp.float32
        ).astype(mix.dtype)
        step = 2 * LANES
        for c in range(0, channels * strip, step):
            full = jnp.dot(picked, spread[:, c : c + step], preferred_element_type=jnp.float32)
            p = lax.broadcasted_iota(jnp.int32, full.shape, 0) % strip
            t = lax.broadcasted_iota(jnp.int32, full.shape, 1) % strip
            kron[:, c : c + step] = jnp.where(p == t, full, 0.0).astype(kron.dtype)

        @pl.loop(0, columns // TILE)
        def _(q):
            cols = pl.ds(pl.multiple_of(q * TILE, TILE), TILE)
            data = x[:, 2, :, cols].reshape(channels * strip, TILE)
            mixed[:, cols] = jnp.dot(kron[...], data, preferred_element_type=jnp.float32)

    def finish(g, column, size):
        cols = pl.ds(column, size)
        data = x[pl.ds(g * width, width), :, :, cols].reshape(width * span, size)
        conv = jnp.dot(band[...], data, preferred_element_type=jnp.float32)
        total = conv + mixed[:, cols]
        for o in range(width):
            c = g * width + o
            value = jax.nn.gelu(total[o * strip : (o + 1) * strip] + bias[c])
            out[c, :, cols] = value.astype(out.dtype)

    @pl.loop(0, groups - 1)
    def _(g):
        build(g)
        part = (g * width, 0, columns, g)
        flow(part, 0).wait_recv()
        flow(part, 1).wait_recv()
        passed(part).start()

        @pl.when(g + LEAD < groups - 1)
        def _():
            later = ((g + LEAD) * width, 0, columns, g + LEAD)
            flow(later, way).start()
            flow(later, 1 - way).start()
            side(later).start()

        @pl.when(g + LEAD == groups - 1)
        def _():
            start_tail(way)
            start_tail(1 - way)
            for later in tail:
                side(later).start()

        side(part).wait_recv()
        passed(part).wait_recv()

        @pl.loop(0, columns // TILE)
        def _(q):
            finish(g, pl.multiple_of(q * TILE, TILE), TILE)

    build(last)
    for q, part in enumerate(tail):
        flow(part, 0).wait_recv()
        flow(part, 1).wait_recv()
        passed(part).start()
        if q > 0:
            side(tail[q - 1]).wait_recv()
            passed(tail[q - 1]).wait_recv()
            finish(last, *tail[q - 1][1:3])
    side(tail[-1]).wait_recv()
    passed(tail[-1]).wait_recv()
    finish(last, *tail[-1][1:3])

    for part in wide + tail:
        flow(part, 0).wait_send()
        flow(part, 1).wait_send()
        side(part).wait_send()
        passed(part).wait_send()

    for j in range(RELAYS):

        @pl.when(relays_up[j] + relays_down[j] == 1)
        def _():
            from_relay(0, j).wait_send()


def local(n, features, row_kernel, mix_weight, channel_bias):
    channels, strip, columns = features.shape
    groups, width, _, tap_count = row_kernel.shape
    strips = (tap_count - 1) // strip + 1
    period = -(-(strips * strip + 3 * strip) // LANES) * LANES
    slots = groups - 1 + len(TAIL)
    small = row_kernel, mix_weight, channel_bias
    hbm = pl.BlockSpec(memory_space=pltpu.HBM)
    return pl.pallas_call(
        functools.partial(kernel, n),
        out_shape=jax.ShapeDtypeStruct(features.shape, jnp.bfloat16),
        in_specs=[hbm, hbm, hbm, hbm],
        out_specs=pl.BlockSpec(memory_space=pltpu.VMEM),
        scratch_shapes=[
            pltpu.VMEM((channels, strips, strip, columns), jnp.bfloat16),
            pltpu.VMEM(row_kernel.shape, jnp.bfloat16),
            pltpu.VMEM((groups, width, width, period), jnp.float32),
            pltpu.VMEM(mix_weight.shape, jnp.bfloat16),
            pltpu.SMEM(channel_bias.shape, jnp.float32),
            pltpu.VMEM((width * strip, width * strips * strip), jnp.bfloat16),
            pltpu.VMEM((width * strip, channels * strip), jnp.bfloat16),
            pltpu.VMEM((channels, channels * strip), jnp.bfloat16),
            pltpu.VMEM((width * strip, columns), jnp.float32),
            pltpu.VMEM((width, strip, max(TAIL[:RELAYS])), jnp.bfloat16),
            pltpu.SemaphoreType.DMA((3,)),
            pltpu.SemaphoreType.DMA((groups,)),
        ]
        + [pltpu.SemaphoreType.DMA((2, slots))] * 2
        + [pltpu.SemaphoreType.DMA((slots,))] * 4
        + [pltpu.SemaphoreType.DMA] * 2
        + [pltpu.SemaphoreType.REGULAR] * 2,
        compiler_params=pltpu.CompilerParams(
            collective_id=0, has_side_effects=True, vmem_limit_bytes=48 * 2**20
        ),
    )(features, *(pltpu.with_memory_space_constraint(a, pltpu.HBM) for a in small))


def solution(mesh):
    return jax.shard_map(
        functools.partial(local, mesh.shape["strip"]),
        mesh=mesh,
        in_specs=(P(None, "strip", None), P(), P(), P()),
        out_specs=P(None, "strip", None),
        check_vma=False,
    )
```
